256 devices in a mesh: tm: 8 (over x, core), rows: 32 (over y, z).
Axes of the slice: x: 4, y: 4, z: 8, core: 2. Of those that a mesh axis runs over, the one named last changes fastest.
Arguments:
- latent: bfloat16 [16, 64, 160, 16], P('tm', 'rows'), may hold values from -6 to 6
- entry_kernel: bfloat16 [3, 3, 3, 16, 256], replicated, may hold values from -0.3125 to 0.3125
- middle_kernel: bfloat16 [3, 3, 3, 256, 256], replicated, may hold values from -0.078125 to 0.078125
- upper_kernel: bfloat16 [3, 3, 3, 256, 256], replicated, may hold values from -0.078125 to 0.078125
Outputs:
- decoded: bfloat16 [16, 128, 320, 256], P('tm', 'rows')
The draws below stay inside these ranges and needn't reach their ends.
All inputs are finite; a program needn't handle non-finite values.
Results may differ from the reference program's by a relative error of at most 0.0059.
Values may be sent and summed in bfloat16 or wider, within the bound.
A program may use at most 64 MiB of HBM per device.

```python
import jax
import jax.numpy as jnp
from jax import lax

CIN = 16
CH = 256
W = 160
NT = 16
NH = 64


def level_of(stream_key, shape, shards, smallest, largest):
    loudness = 1.0
    for axis_at, parts in shards:
        steps = jax.random.uniform(jax.random.fold_in(jax.random.fold_in(stream_key, 6), axis_at), (parts,), jnp.float32, smallest / len(shards), largest / len(shards))
        loudness = loudness * jnp.repeat(jnp.exp(steps), shape[axis_at] // parts).reshape((-1,) + (1,) * (len(shape) - 1 - axis_at))
    return loudness


def centred(own_key, extent, width, bound, pieces=(), held_as=jnp.bfloat16):
    array = width * jax.random.normal(own_key, extent, jnp.float32)
    if pieces:
        array = array * level_of(own_key, extent, pieces, -0.22, 0.18)
    return jnp.clip(array, -bound, bound).astype(held_as)


def setup_inputs(seed: int = 0) -> dict:
    arg_keys = jax.random.split(jax.random.key(seed), 5)
    return {
        "latent": centred(arg_keys[0], (NT, NH, W, CIN), 1.0, 6.0, ((0, 8), (1, 32))),
        "entry_kernel": centred(arg_keys[1], (3, 3, 3, CIN, CH), (27 * CIN) ** -0.5, 0.3125),
        "middle_kernel": centred(arg_keys[2], (3, 3, 3, CH, CH), (27 * CH) ** -0.5, 0.078125),
        "upper_kernel": centred(arg_keys[3], (3, 3, 3, CH, CH), (27 * CH) ** -0.5, 0.078125),
    }


def convolve(field, weight):
    result = lax.conv_general_dilated(field.astype(jnp.float32)[None], weight.astype(jnp.float32), (1, 1, 1), [(2, 0), (1, 1), (1, 1)], dimension_numbers=("NDHWC", "DHWIO", "NDHWC"))
    return result[0]


def reference(latent, entry_kernel, middle_kernel, upper_kernel):
    bottom = convolve(latent, entry_kernel).astype(jnp.bfloat16)
    middle = convolve(bottom, middle_kernel)
    section_one = (bottom.astype(jnp.float32) + jax.nn.silu(middle)).astype(jnp.bfloat16)
    enlarged = jnp.repeat(jnp.repeat(section_one, 2, axis=1), 2, axis=2)
    return jax.nn.silu(convolve(enlarged, upper_kernel)).astype(jnp.bfloat16)
```

```python
import jax
import jax.numpy as jnp
from jax import lax
from jax.experimental import pallas as pl
from jax.experimental.pallas import tpu as pltpu
from jax.sharding import PartitionSpec as P

F32 = jnp.float32
BF = jnp.bfloat16
W = 160
C = 256
CI = 16
NBACK = 3
NSIDE = 2


def roll_cols(x, d):
    n = x.shape[0]
    row = lax.broadcasted_iota(jnp.int32, x.shape, 0)
    if d == 0:
        return jnp.where(row == 0, 0.0, pltpu.roll(x, 1, 0))
    return jnp.where(row == n - 1, 0.0, pltpu.roll(x, n - 1, 0))


def silu(v):
    return v * (1.0 / (1.0 + jnp.exp(-v)))


def put3(dst, idx, x):
    for d in range(3):
        y = x if d == 1 else roll_cols(x, d)
        dst[(d,) + idx] = y.astype(BF)


def partners():
    return [(i, j) for i in range(NBACK + 1) for j in range(-NSIDE, NSIDE + 1) if (i, j) != (0, 0)]


def exchange_body(nt, nr, lat, ek, uk, R, WE, WU, ubuf, usem, ssem, rsem):
    me_t = lax.axis_index("tm")
    me_r = lax.axis_index("rows")

    def there(di, dj):
        t = me_t + di
        r = me_r + dj
        return (t >= 0) & (t < nt) & (r >= 0) & (r < nr)

    def to(di, dj):
        return {"tm": me_t + di, "rows": me_r + dj}

    load = pltpu.make_async_copy(uk, ubuf, usem)
    load.start()
    barrier = pltpu.get_barrier_semaphore()
    for i, j in partners():
        @pl.when(there(-i, -j))
        def _():
            pl.semaphore_signal(barrier, inc=1, device_id=to(-i, -j), device_id_type=pl.DeviceIdType.MESH)
    R[6:8, 3:5] = lat[...]
    slots = {-2: (7, 8), -1: (5, 7), 0: (3, 5), 1: (1, 3), 2: (0, 1)}
    for i, j in partners():
        lo, hi = slots[j]

        @pl.when(jnp.logical_not(there(-i, -j)))
        def _():
            R[6 - 2 * i:8 - 2 * i, lo:hi] = jnp.zeros((2, hi - lo, CI, W), BF)
    ahead = jnp.minimum(nt - 1 - me_t, NBACK) + 1
    beside = jnp.minimum(me_r, NSIDE) + jnp.minimum(nr - 1 - me_r, NSIDE) + 1
    pl.semaphore_wait(barrier, ahead * beside - 1)

    def copy(n, i, j):
        lo, hi = slots[j]
        if j == 2:
            src = lat.at[:, 1:2]
        elif j == -2:
            src = lat.at[:, 0:1]
        else:
            src = lat
        return pltpu.make_async_remote_copy(
            src_ref=src,
            dst_ref=R.at[6 - 2 * i:8 - 2 * i, lo:hi],
            send_sem=ssem.at[n],
            recv_sem=rsem.at[n],
            device_id=to(i, j),
            device_id_type=pl.DeviceIdType.MESH,
        )

    for n, (i, j) in enumerate(partners()):
        @pl.when(there(i, j))
        def _():
            copy(n, i, j).start()

    WE[...] = jnp.zeros(WE.shape, BF)
    for dc in range(3):
        for dt in range(3):
            for dr in range(3):
                w = ek[dt, dr, dc]
                for fo in range(2):
                    for ro in range(2):
                        k = ((fo + dt) * 4 + ro + dr) * CI
                        n = (fo * 2 + ro) * C
                        WE[dc, k:k + CI, n:n + C] = w
    load.wait()

    def fold(s, carry):
        dt = s // 8
        r0 = pl.multiple_of((s % 8) * 32, 32)
        m = [[ubuf[dt, r, c, pl.ds(r0, 32), :].astype(F32) for c in range(3)] for r in range(3)]
        rows = [[m[0], [m[1][c] + m[2][c] for c in range(3)]],
                [[m[0][c] + m[1][c] for c in range(3)], m[2]]]
        for a in range(2):
            for e in range(2):
                q = rows[a][e]
                cols = [[q[0], q[1] + q[2]], [q[0] + q[1], q[2]]]
                for b in range(2):
                    for c in range(2):
                        WU[a, b, dt, e, c, pl.ds(r0, 32), :] = cols[b][c].astype(BF)
        return carry

    lax.fori_loop(0, 24, fold, 0)

    for n, (i, j) in enumerate(partners()):
        @pl.when(there(i, j))
        def _():
            copy(n, i, j).wait_send()

        @pl.when(there(-i, -j))
        def _():
            copy(n, i, j).wait_recv()


def exchange(nt, nr, lat, ek, uk):
    vm = pl.BlockSpec(memory_space=pltpu.VMEM)
    n = len(partners())

    def body(*refs):
        exchange_body(nt, nr, *refs)

    return pl.pallas_call(
        body,
        out_shape=(
            jax.ShapeDtypeStruct((8, 8, CI, W), BF),
            jax.ShapeDtypeStruct((3, 256, 1024), BF),
            jax.ShapeDtypeStruct((2, 2, 3, 2, 2, C, C), BF),
        ),
        in_specs=[vm, vm, pl.BlockSpec(memory_space=pl.ANY)],
        out_specs=(vm, vm, vm),
        scratch_shapes=[
            pltpu.VMEM((3, 3, 3, C, C), BF),
            pltpu.SemaphoreType.DMA,
            pltpu.SemaphoreType.DMA((n,)),
            pltpu.SemaphoreType.DMA((n,)),
        ],
        compiler_params=pltpu.CompilerParams(collective_id=0, has_side_effects=True, vmem_limit_bytes=16 * 2**20),
        name="exchange",
    )(lat, ek, uk)


def decode_body(n_rows, height, R, WE, W2, WU, out, V, B3, S3, I):
    row_base = lax.axis_index("rows") * height
    for g in range(3):
        for fp in range(4):
            y = R[2 * fp:2 * fp + 2, 2 * g:2 * g + 4].reshape(128, W).astype(F32).T
            for d in range(3):
                z = y if d == 1 else roll_cols(y, d)
                V[d, g, fp] = z.astype(BF)
    for g in range(3):
        for fo in range(2):
            acc = None
            for d in range(3):
                lhs = jnp.concatenate(
                    [jnp.concatenate([V[d, g, k], V[d, g, k + 1]], axis=1) for k in range(3)], axis=0)
                p = jnp.dot(lhs, WE[d, :, fo * 512:(fo + 1) * 512], preferred_element_type=F32)
                acc = p if acc is None else acc + p
            for ro in range(2):
                gr = row_base - 2 + 2 * g + ro
                ok = jnp.where((gr >= 0) & (gr < n_rows), 1.0, 0.0)
                for k in range(3):
                    put3(B3, (2 * k + fo, 2 * g + ro), acc[k * W:(k + 1) * W, ro * C:(ro + 1) * C] * ok)

    def mid(f, carry):
        acc = None
        for dt in range(3):
            for dr in range(3):
                for dc in range(3):
                    lhs = B3[dc, f + dt, dr:dr + 4].reshape(4 * W, C)
                    p = jnp.dot(lhs, W2[dt, dr, dc], preferred_element_type=F32)
                    acc = p if acc is None else acc + p
        for r in range(4):
            gr = row_base - 1 + r
            ok = jnp.where((gr >= 0) & (gr < n_rows), 1.0, 0.0)
            s = (B3[1, f + 2, r + 1].astype(F32) + silu(acc[r * W:(r + 1) * W])) * ok
            put3(S3, (f, r), s)
        return carry

    lax.fori_loop(0, 4, mid, 0)
    for a in range(2):
        for b in range(2):
            acc = None
            for dt in range(3):
                for e in range(2):
                    for c in range(2):
                        lhs = jnp.concatenate(
                            [S3[b + c, t + dt, a + e + q] for t in range(2) for q in range(2)], axis=0)
                        p = jnp.dot(lhs, WU[a, b, dt, e, c], preferred_element_type=F32)
                        acc = p if acc is None else acc + p
            y = silu(acc)
            for i in range(4):
                for h in range(2):
                    I[i, h, pl.ds(b, W, stride=2), :] = y[i * W:(i + 1) * W, h * 128:(h + 1) * 128]
        for i in range(4):
            for h in range(2):
                out[i // 2, 2 * (i % 2) + a, :, h * 128:(h + 1) * 128] = I[i, h].astype(BF)


def decode(n_rows, height, R, WE, W2, WU):
    vm = pl.BlockSpec(memory_space=pltpu.VMEM)

    def body(*refs):
        decode_body(n_rows, height, *refs)

    return pl.pallas_call(
        body,
        out_shape=jax.ShapeDtypeStruct((2, 4, 2 * W, C), BF),
        in_specs=[vm, vm, vm, vm],
        out_specs=vm,
        scratch_shapes=[
            pltpu.VMEM((3, 3, 4, W, 128), BF),
            pltpu.VMEM((3, 6, 6, W, C), BF),
            pltpu.VMEM((3, 4, 4, W, C), BF),
            pltpu.VMEM((4, 2, 2 * W, 128), F32),
        ],
        compiler_params=pltpu.CompilerParams(vmem_limit_bytes=40 * 2**20),
        name="decode",
    )(R, WE, W2, WU)


def per_device(nt, nr, latent, entry_kernel, middle_kernel, upper_kernel):
    height = latent.shape[1]
    lat = jnp.transpose(latent, (0, 1, 3, 2))
    R, WE, WU = exchange(nt, nr, lat, entry_kernel, pltpu.with_memory_space_constraint(upper_kernel, pltpu.HBM))
    return decode(height * nr, height, R, WE, middle_kernel, WU)


def solution(mesh):
    nt = mesh.shape["tm"]
    nr = mesh.shape["rows"]
    return jax.shard_map(
        lambda *a: per_device(nt, nr, *a),
        mesh=mesh,
        in_specs=(P("tm", "rows", None, None), P(), P(), P()),
        out_specs=P("tm", "rows", None, None),
        check_vma=False,
    )
```

```python
import jax
import jax.numpy as jnp
from jax import lax
from jax.experimental import pallas as pl
from jax.experimental.pallas import tpu as pltpu
from jax.sharding import PartitionSpec as P

F32 = jnp.float32
BF = jnp.bfloat16
W = 160
C = 256
CI = 16
NBACK = 3
NSIDE = 2


def roll_cols(x, d):
    n = x.shape[0]
    row = lax.broadcasted_iota(jnp.int32, x.shape, 0)
    if d == 0:
        return jnp.where(row == 0, 0.0, pltpu.roll(x, 1, 0))
    return jnp.where(row == n - 1, 0.0, pltpu.roll(x, n - 1, 0))


def silu(v):
    return v * (1.0 / (1.0 + jnp.exp(-v)))


def put3(dst, idx, x):
    for d in range(3):
        y = x if d == 1 else roll_cols(x, d)
        dst[(d,) + idx] = y.astype(BF)


def partners():
    return [(i, j) for i in range(NBACK + 1) for j in range(-NSIDE, NSIDE + 1) if (i, j) != (0, 0)]


ROW_OF = ((0, 1), (1, 0), (1, 1), (2, 0), (2, 1), (3, 0), (3, 1), (4, 0))


def exchange_body(nt, nr, lat_h, ek_h, uk, R, WE, WU, lat, ek, ubuf, pack, lsem, ssem, rsem):
    me_t = lax.axis_index("tm")
    me_r = lax.axis_index("rows")

    def there(di, dj):
        t = me_t + di
        r = me_r + dj
        return (t >= 0) & (t < nt) & (r >= 0) & (r < nr)

    def to(di, dj):
        return {"tm": me_t + di, "rows": me_r + dj}

    loads = [pltpu.make_async_copy(src, dst, lsem.at[n])
             for n, (src, dst) in enumerate(((lat_h, lat), (ek_h, ek), (uk, ubuf)))]
    for x in loads:
        x.start()
    barrier = pltpu.get_barrier_semaphore()
    for i, j in partners():
        @pl.when(there(-i, -j))
        def _():
            pl.semaphore_signal(barrier, inc=1, device_id=to(-i, -j), device_id_type=pl.DeviceIdType.MESH)
    for i, j in partners():
        @pl.when(jnp.logical_not(there(-i, -j)))
        def _():
            R[NBACK - i, 2 - j] = jnp.zeros((5, CI, 128), BF)
    loads[0].wait()
    tails = []
    for r in range(2):
        for f in range(2):
            v = lat[f, r]
            pack[3 * r + f] = v[:, :128]
            tails.append(v[:, 128:].astype(F32))
    pack[2] = jnp.concatenate(tails, axis=1).astype(BF)
    R[NBACK, 2] = pack[...]
    ahead = jnp.minimum(nt - 1 - me_t, NBACK) + 1
    beside = jnp.minimum(me_r, NSIDE) + jnp.minimum(nr - 1 - me_r, NSIDE) + 1
    pl.semaphore_wait(barrier, ahead * beside - 1)

    def copy(n, i, j):
        lo, hi = {2: (2, 5), -2: (0, 3)}.get(j, (0, 5))
        return pltpu.make_async_remote_copy(
            src_ref=pack.at[lo:hi],
            dst_ref=R.at[NBACK - i, 2 - j, lo:hi],
            send_sem=ssem.at[n],
            recv_sem=rsem.at[n],
            device_id=to(i, j),
            device_id_type=pl.DeviceIdType.MESH,
        )

    for n, (i, j) in enumerate(partners()):
        @pl.when(there(i, j))
        def _():
            copy(n, i, j).start()

    WE[...] = jnp.zeros(WE.shape, BF)
    loads[1].wait()
    for dc in range(3):
        for dt in range(3):
            for dr in range(3):
                w = ek[dt, dr, dc]
                for fo in range(2):
                    for ro in range(2):
                        k = ((fo + dt) * 4 + ro + dr) * CI
                        n = (fo * 2 + ro) * C
                        WE[dc, k:k + CI, n:n + C] = w
    loads[2].wait()

    def fold(s, carry):
        dt = s // 8
        r0 = pl.multiple_of((s % 8) * 32, 32)
        m = [[ubuf[dt, r, c, pl.ds(r0, 32), :].astype(F32) for c in range(3)] for r in range(3)]
        rows = [[m[0], [m[1][c] + m[2][c] for c in range(3)]],
                [[m[0][c] + m[1][c] for c in range(3)], m[2]]]
        for a in range(2):
            for e in range(2):
                q = rows[a][e]
                cols = [[q[0], q[1] + q[2]], [q[0] + q[1], q[2]]]
                for b in range(2):
                    for c in range(2):
                        WU[a, b, dt, e, c, pl.ds(r0, 32), :] = cols[b][c].astype(BF)
        return carry

    lax.fori_loop(0, 24, fold, 0)

    for n, (i, j) in enumerate(partners()):
        @pl.when(there(i, j))
        def _():
            copy(n, i, j).wait_send()

        @pl.when(there(-i, -j))
        def _():
            copy(n, i, j).wait_recv()


def exchange(nt, nr, lat, ek, uk):
    vm = pl.BlockSpec(memory_space=pltpu.VMEM)
    hbm = pl.BlockSpec(memory_space=pl.ANY)
    n = len(partners())

    def body(*refs):
        exchange_body(nt, nr, *refs)

    return pl.pallas_call(
        body,
        out_shape=(
            jax.ShapeDtypeStruct((4, 5, 5, CI, 128), BF),
            jax.ShapeDtypeStruct((3, 256, 1024), BF),
            jax.ShapeDtypeStruct((2, 2, 3, 2, 2, C, C), BF),
        ),
        in_specs=[hbm, hbm, hbm],
        out_specs=(vm, vm, vm),
        scratch_shapes=[
            pltpu.VMEM((2, 2, CI, W), BF),
            pltpu.VMEM((3, 3, 3, CI, C), BF),
            pltpu.VMEM((3, 3, 3, C, C), BF),
            pltpu.VMEM((5, CI, 128), BF),
            pltpu.SemaphoreType.DMA((3,)),
            pltpu.SemaphoreType.DMA((n,)),
            pltpu.SemaphoreType.DMA((n,)),
        ],
        compiler_params=pltpu.CompilerParams(collective_id=0, has_side_effects=True, vmem_limit_bytes=16 * 2**20),
        name="exchange",
    )(*[pltpu.with_memory_space_constraint(x, pltpu.HBM) for x in (lat, ek, uk)])


def window(R, fp, g):
    main, tail = [], []
    for f in range(2):
        for w in range(4):
            b, r = ROW_OF[2 * g + w]
            main.append(R[fp, b, 3 * r + f].astype(F32))
            k = 32 * (2 * r + f)
            tail.append(R[fp, b, 2].astype(F32)[:, k:k + 32])
    return jnp.concatenate([jnp.concatenate(main, axis=0).T, jnp.concatenate(tail, axis=0).T], axis=0)


def decode_body(n_rows, height, R, WE, W2, WU, out, V, B3, S3, I):
    row_base = lax.axis_index("rows") * height
    for g in range(3):
        for fp in range(4):
            y = window(R, fp, g)
            for d in range(3):
                z = y if d == 1 else roll_cols(y, d)
                V[d, g, fp] = z.astype(BF)
    for g in range(3):
        for fo in range(2):
            acc = None
            for d in range(3):
                lhs = jnp.concatenate(
                    [jnp.concatenate([V[d, g, k], V[d, g, k + 1]], axis=1) for k in range(3)], axis=0)
                p = jnp.dot(lhs, WE[d, :, fo * 512:(fo + 1) * 512], preferred_element_type=F32)
                acc = p if acc is None else acc + p
            for ro in range(2):
                gr = row_base - 2 + 2 * g + ro
                ok = jnp.where((gr >= 0) & (gr < n_rows), 1.0, 0.0)
                for k in range(3):
                    put3(B3, (2 * k + fo, 2 * g + ro), acc[k * W:(k + 1) * W, ro * C:(ro + 1) * C] * ok)

    def mid(f, carry):
        acc = None
        for dt in range(3):
            for dr in range(3):
                for dc in range(3):
                    lhs = B3[dc, f + dt, dr:dr + 4].reshape(4 * W, C)
                    p = jnp.dot(lhs, W2[dt, dr, dc], preferred_element_type=F32)
                    acc = p if acc is None else acc + p
        for r in range(4):
            gr = row_base - 1 + r
            ok = jnp.where((gr >= 0) & (gr < n_rows), 1.0, 0.0)
            s = (B3[1, f + 2, r + 1].astype(F32) + silu(acc[r * W:(r + 1) * W])) * ok
            put3(S3, (f, r), s)
        return carry

    lax.fori_loop(0, 4, mid, 0)
    for a in range(2):
        for b in range(2):
            acc = None
            for dt in range(3):
                for e in range(2):
                    for c in range(2):
                        lhs = jnp.concatenate(
                            [S3[b + c, t + dt, a + e + q] for t in range(2) for q in range(2)], axis=0)
                        p = jnp.dot(lhs, WU[a, b, dt, e, c], preferred_element_type=F32)
                        acc = p if acc is None else acc + p
            y = silu(acc)
            for i in range(4):
                for h in range(2):
                    I[i, h, pl.ds(b, W, stride=2), :] = y[i * W:(i + 1) * W, h * 128:(h + 1) * 128]
        for i in range(4):
            for h in range(2):
                out[i // 2, 2 * (i % 2) + a, :, h * 128:(h + 1) * 128] = I[i, h].astype(BF)


def decode(n_rows, height, R, WE, W2, WU):
    vm = pl.BlockSpec(memory_space=pltpu.VMEM)

    def body(*refs):
        decode_body(n_rows, height, *refs)

    return pl.pallas_call(
        body,
        out_shape=jax.ShapeDtypeStruct((2, 4, 2 * W, C), BF),
        in_specs=[vm, vm, vm, vm],
        out_specs=vm,
        scratch_shapes=[
            pltpu.VMEM((3, 3, 4, W, 128), BF),
            pltpu.VMEM((3, 6, 6, W, C), BF),
            pltpu.VMEM((3, 4, 4, W, C), BF),
            pltpu.VMEM((4, 2, 2 * W, 128), F32),
        ],
        compiler_params=pltpu.CompilerParams(vmem_limit_bytes=40 * 2**20),
        name="decode",
    )(R, WE, W2, WU)


def per_device(nt, nr, latent, entry_kernel, middle_kernel, upper_kernel):
    height = latent.shape[1]
    lat = jnp.transpose(latent, (0, 1, 3, 2))
    R, WE, WU = exchange(nt, nr, lat, entry_kernel, upper_kernel)
    return decode(height * nr, height, R, WE, middle_kernel, WU)


def solution(mesh):
    nt = mesh.shape["tm"]
    nr = mesh.shape["rows"]
    return jax.shard_map(
        lambda *a: per_device(nt, nr, *a),
        mesh=mesh,
        in_specs=(P("tm", "rows", None, None), P(), P(), P()),
        out_specs=P("tm", "rows", None, None),
        check_vma=False,
    )
```

```python
import jax
import jax.numpy as jnp
from jax import lax
from jax.experimental import pallas as pl
from jax.experimental.pallas import tpu as pltpu
from jax.sharding import PartitionSpec as P

F32 = jnp.float32
BF = jnp.bfloat16
W = 160
C = 256
CI = 16
NBACK = 3
NSIDE = 2


def roll_cols(x, d):
    n = x.shape[0]
    row = lax.broadcasted_iota(jnp.int32, x.shape, 0)
    if d == 0:
        return jnp.where(row == 0, 0.0, pltpu.roll(x, 1, 0))
    return jnp.where(row == n - 1, 0.0, pltpu.roll(x, n - 1, 0))


def silu(v):
    h = 0.5 * v
    return h + h * jnp.tanh(h)


def put3(dst, idx, x):
    for d in range(3):
        y = x if d == 1 else roll_cols(x, d)
        dst[(d,) + idx] = y.astype(BF)


def partners():
    return [(i, j) for i in range(NBACK + 1) for j in range(-NSIDE, NSIDE + 1) if (i, j) != (0, 0)]


ROW_OF = ((0, 1), (1, 0), (1, 1), (2, 0), (2, 1), (3, 0), (3, 1), (4, 0))


def exchange_body(nt, nr, lat_h, ek_h, uk, mk, R, WE, W2, WM, WU, lat, ek, ubuf, pack, lsem, ssem, rsem):
    me_t = lax.axis_index("tm")
    me_r = lax.axis_index("rows")

    def there(di, dj):
        t = me_t + di
        r = me_r + dj
        return (t >= 0) & (t < nt) & (r >= 0) & (r < nr)

    def to(di, dj):
        return {"tm": me_t + di, "rows": me_r + dj}

    loads = [pltpu.make_async_copy(src, dst, lsem.at[n])
             for n, (src, dst) in enumerate(((lat_h, lat), (ek_h, ek), (uk, ubuf), (mk, W2)))]
    for x in loads:
        x.start()
    barrier = pltpu.get_barrier_semaphore()
    for i, j in partners():
        @pl.when(there(-i, -j))
        def _():
            pl.semaphore_signal(barrier, inc=1, device_id=to(-i, -j), device_id_type=pl.DeviceIdType.MESH)
    for i, j in partners():
        @pl.when(jnp.logical_not(there(-i, -j)))
        def _():
            R[NBACK - i, 2 - j] = jnp.zeros((5, CI, 128), BF)
    loads[0].wait()
    tails = []
    for r in range(2):
        for f in range(2):
            v = lat[f, r]
            pack[3 * r + f] = v[:, :128]
            tails.append(v[:, 128:].astype(F32))
    pack[2] = jnp.concatenate(tails, axis=1).astype(BF)
    R[NBACK, 2] = pack[...]
    ahead = jnp.minimum(nt - 1 - me_t, NBACK) + 1
    beside = jnp.minimum(me_r, NSIDE) + jnp.minimum(nr - 1 - me_r, NSIDE) + 1
    pl.semaphore_wait(barrier, ahead * beside - 1)

    def copy(n, i, j):
        lo, hi = {2: (2, 5), -2: (0, 3)}.get(j, (0, 5))
        return pltpu.make_async_remote_copy(
            src_ref=pack.at[lo:hi],
            dst_ref=R.at[NBACK - i, 2 - j, lo:hi],
            send_sem=ssem.at[n],
            recv_sem=rsem.at[n],
            device_id=to(i, j),
            device_id_type=pl.DeviceIdType.MESH,
        )

    for n, (i, j) in reversed(list(enumerate(partners()))):
        @pl.when(there(i, j))
        def _():
            copy(n, i, j).start()

    WE[...] = jnp.zeros(WE.shape, BF)
    loads[1].wait()
    for dc in range(3):
        for dt in range(3):
            for dr in range(3):
                w = ek[dt, dr, dc]
                for fo in range(2):
                    for ro in range(2):
                        k = ((fo + dt) * 4 + ro + dr) * CI
                        n = (fo * 2 + ro) * C
                        WE[dc, k:k + CI, n:n + C] = w
    loads[2].wait()
    loads[3].wait()

    def fold(s, carry):
        dt = s // 8
        r0 = pl.multiple_of((s % 8) * 32, 32)
        m = [[ubuf[dt, r, c, pl.ds(r0, 32), :].astype(F32) for c in range(3)] for r in range(3)]
        rows = [m[0], [m[0][c] + m[1][c] + m[2][c] for c in range(3)], m[2]]
        for a in range(3):
            q = rows[a]
            cols = [[q[0], q[1] + q[2]], [q[0] + q[1], q[2]]]
            for b in range(2):
                for c in range(2):
                    WU[a, b, dt, c, pl.ds(r0, 32), :] = cols[b][c].astype(BF)
        dr = dt
        for dc in range(3):
            k = [W2[t, dr, dc, pl.ds(r0, 32), :].astype(F32) for t in range(3)]
            half = 0.5 * (k[0] + k[2])
            one = 0.5 * k[1]
            WM[0, dr, dc, pl.ds(r0, 32), :] = (half + one).astype(BF)
            WM[1, dr, dc, pl.ds(r0, 32), :] = (half - one).astype(BF)
        return carry

    lax.fori_loop(0, 24, fold, 0)

    for n, (i, j) in enumerate(partners()):
        @pl.when(there(i, j))
        def _():
            copy(n, i, j).wait_send()

        @pl.when(there(-i, -j))
        def _():
            copy(n, i, j).wait_recv()


def exchange(nt, nr, lat, ek, uk, mk):
    vm = pl.BlockSpec(memory_space=pltpu.VMEM)
    hbm = pl.BlockSpec(memory_space=pl.ANY)
    n = len(partners())

    def body(*refs):
        exchange_body(nt, nr, *refs)

    return pl.pallas_call(
        body,
        out_shape=(
            jax.ShapeDtypeStruct((4, 5, 5, CI, 128), BF),
            jax.ShapeDtypeStruct((3, 256, 1024), BF),
            jax.ShapeDtypeStruct((3, 3, 3, C, C), BF),
            jax.ShapeDtypeStruct((2, 3, 3, C, C), BF),
            jax.ShapeDtypeStruct((3, 2, 3, 2, C, C), BF),
        ),
        in_specs=[hbm] * 4,
        out_specs=(vm,) * 5,
        scratch_shapes=[
            pltpu.VMEM((2, 2, CI, W), BF),
            pltpu.VMEM((3, 3, 3, CI, C), BF),
            pltpu.VMEM((3, 3, 3, C, C), BF),
            pltpu.VMEM((5, CI, 128), BF),
            pltpu.SemaphoreType.DMA((4,)),
            pltpu.SemaphoreType.DMA((n,)),
            pltpu.SemaphoreType.DMA((n,)),
        ],
        compiler_params=pltpu.CompilerParams(collective_id=0, has_side_effects=True, vmem_limit_bytes=16 * 2**20),
        name="exchange",
    )(*[pltpu.with_memory_space_constraint(x, pltpu.HBM) for x in (lat, ek, uk, mk)])


def window(R, fp, g):
    main, tail = [], []
    for f in range(2):
        for w in range(4):
            b, r = ROW_OF[2 * g + w]
            main.append(R[fp, b, 3 * r + f].astype(F32))
            k = 32 * (2 * r + f)
            tail.append(R[fp, b, 2].astype(F32)[:, k:k + 32])
    return jnp.concatenate([jnp.concatenate(main, axis=0).T, jnp.concatenate(tail, axis=0).T], axis=0)


FRAMES = ((0, 2, -1), (1, 2, 1), (2, 1, -1), (1, 3, -1))


def decode_body(n_rows, height, R, WE, W2, WM, WU, out, V, B3, S3, I, CR, MID):
    row_base = lax.axis_index("rows") * height

    def inside(r):
        return jnp.where((r >= 0) & (r < n_rows), 1.0, 0.0)

    for g in range(3):
        for fp in range(4):
            y = window(R, fp, g)
            for d in range(3):
                z = y if d == 1 else roll_cols(y, d)
                V[d, g, fp] = z.astype(BF)
    for g in range(3):
        for fo in range(2):
            acc = None
            for d in range(3):
                lhs = jnp.concatenate(
                    [jnp.concatenate([V[d, g, k], V[d, g, k + 1]], axis=1) for k in range(3)], axis=0)
                p = jnp.dot(lhs, WE[d, :, fo * 512:(fo + 1) * 512], preferred_element_type=F32)
                acc = p if acc is None else acc + p
            for ro in range(2):
                ok = inside(row_base - 2 + 2 * g + ro)
                for k in range(3):
                    put3(B3, (2 * k + fo, 2 * g + ro), acc[k * W:(k + 1) * W, ro * C:(ro + 1) * C] * ok)

    for p in range(2):
        f0 = 2 * p
        for i in range(4):
            fa, fb, sign = FRAMES[i]
            acc = None
            for dr in range(3):
                for dc in range(3):
                    u = B3[dc, f0 + fa, dr:dr + 4].reshape(4 * W, C)
                    v = B3[dc, f0 + fb, dr:dr + 4].reshape(4 * W, C)
                    lhs = u + v if sign > 0 else u - v
                    w = W2[0, dr, dc] if i == 0 else W2[2, dr, dc] if i == 3 else WM[i - 1, dr, dc]
                    q = jnp.dot(lhs, w, preferred_element_type=F32)
                    acc = q if acc is None else acc + q
            if i == 0:
                MID[0] = acc
            elif i == 1:
                MID[0] = MID[0] + acc
                MID[1] = acc
            else:
                t = i - 2
                if t == 0:
                    y = MID[0] + acc
                    MID[1] = MID[1] - acc
                else:
                    y = MID[1] - acc
                for r in range(4):
                    s = (B3[1, f0 + t + 2, r + 1].astype(F32) + silu(y[r * W:(r + 1) * W])) * inside(row_base - 1 + r)
                    put3(S3, (f0 + t, r), s)

    def prod(a, b):
        acc = None
        for dt in range(3):
            for c in range(2):
                parts = []
                for t in range(2):
                    for q in range(2):
                        x = [S3[b + c, t + dt, q + k] for k in ((0, 1), (1,), (1, 2))[a]]
                        parts.append(x[0] if a == 1 else x[0] - x[1] if a == 0 else x[1] - x[0])
                p = jnp.dot(jnp.concatenate(parts, axis=0), WU[a, b, dt, c], preferred_element_type=F32)
                acc = p if acc is None else acc + p
        return acc

    for b in range(2):
        CR[b] = prod(1, b)
    for a in range(2):
        for b in range(2):
            y = silu(prod(2 * a, b) + CR[b])
            for i in range(4):
                for h in range(2):
                    I[i, h, pl.ds(b, W, stride=2), :] = y[i * W:(i + 1) * W, h * 128:(h + 1) * 128]
        for i in range(4):
            for h in range(2):
                out[i // 2, 2 * (i % 2) + a, :, h * 128:(h + 1) * 128] = I[i, h].astype(BF)


def decode(n_rows, height, *operands):
    vm = pl.BlockSpec(memory_space=pltpu.VMEM)

    def body(*refs):
        decode_body(n_rows, height, *refs)

    return pl.pallas_call(
        body,
        out_shape=jax.ShapeDtypeStruct((2, 4, 2 * W, C), BF),
        in_specs=[vm] * len(operands),
        out_specs=vm,
        scratch_shapes=[
            pltpu.VMEM((3, 3, 4, W, 128), BF),
            pltpu.VMEM((3, 6, 6, W, C), BF),
            pltpu.VMEM((3, 4, 4, W, C), BF),
            pltpu.VMEM((4, 2, 2 * W, 128), F32),
            pltpu.VMEM((2, 4 * W, C), F32),
            pltpu.VMEM((2, 4 * W, C), F32),
        ],
        compiler_params=pltpu.CompilerParams(vmem_limit_bytes=32 * 2**20),
        name="decode",
    )(*operands)


def per_device(nt, nr, latent, entry_kernel, middle_kernel, upper_kernel):
    height = latent.shape[1]
    lat = jnp.transpose(latent, (0, 1, 3, 2))
    return decode(height * nr, height, *exchange(nt, nr, lat, entry_kernel, upper_kernel, middle_kernel))


def solution(mesh):
    nt = mesh.shape["tm"]
    nr = mesh.shape["rows"]
    return jax.shard_map(
        lambda *a: per_device(nt, nr, *a),
        mesh=mesh,
        in_specs=(P("tm", "rows", None, None), P(), P(), P()),
        out_specs=P("tm", "rows", None, None),
        check_vma=False,
    )
```

```python
import jax
import jax.numpy as jnp
from jax import lax
from jax.experimental import pallas as pl
from jax.experimental.pallas import tpu as pltpu
from jax.sharding import PartitionSpec as P

F32 = jnp.float32
BF = jnp.bfloat16
W = 160
C = 256
CI = 16
NBACK = 3
NSIDE = 2


def roll_cols(x, d):
    n = x.shape[0]
    row = lax.broadcasted_iota(jnp.int32, x.shape, 0)
    if d == 0:
        return jnp.where(row == 0, 0.0, pltpu.roll(x, 1, 0))
    return jnp.where(row == n - 1, 0.0, pltpu.roll(x, n - 1, 0))


def silu(v):
    h = 0.5 * v
    return h + h * jnp.tanh(h)


def put3(dst, idx, x):
    for d in range(3):
        y = x if d == 1 else roll_cols(x, d)
        dst[(d,) + idx] = y.astype(BF)


def partners():
    return [(i, j) for i in range(NBACK + 1) for j in range(-NSIDE, NSIDE + 1) if (i, j) != (0, 0)]


ROW_OF = ((0, 1), (1, 0), (1, 1), (2, 0), (2, 1), (3, 0), (3, 1), (4, 0))


def section_body(nt, nr, height, lat_h, ek_h, uk, mk, out, R, WE, W2, WM, WU, V, B3, S3, I, CR, MID, lat, ek, ubuf, pack, lsem, ssem, rsem):
    me_t = lax.axis_index("tm")
    me_r = lax.axis_index("rows")

    def there(di, dj):
        t = me_t + di
        r = me_r + dj
        return (t >= 0) & (t < nt) & (r >= 0) & (r < nr)

    def to(di, dj):
        return {"tm": me_t + di, "rows": me_r + dj}

    loads = [pltpu.make_async_copy(src, dst, lsem.at[n])
             for n, (src, dst) in enumerate(((lat_h, lat), (ek_h, ek), (uk, ubuf), (mk, W2)))]
    for x in loads:
        x.start()
    barrier = pltpu.get_barrier_semaphore()
    for i, j in partners():
        @pl.when(there(-i, -j))
        def _():
            pl.semaphore_signal(barrier, inc=1, device_id=to(-i, -j), device_id_type=pl.DeviceIdType.MESH)
    for i, j in partners():
        @pl.when(jnp.logical_not(there(-i, -j)))
        def _():
            R[NBACK - i, 2 - j] = jnp.zeros((5, CI, 128), BF)
    loads[0].wait()
    tails = []
    for r in range(2):
        for f in range(2):
            v = lat[f, r]
            pack[3 * r + f] = v[:, :128]
            tails.append(v[:, 128:].astype(F32))
    pack[2] = jnp.concatenate(tails, axis=1).astype(BF)
    R[NBACK, 2] = pack[...]
    ahead = jnp.minimum(nt - 1 - me_t, NBACK) + 1
    beside = jnp.minimum(me_r, NSIDE) + jnp.minimum(nr - 1 - me_r, NSIDE) + 1
    pl.semaphore_wait(barrier, ahead * beside - 1)

    def copy(n, i, j):
        lo, hi = {2: (2, 5), -2: (0, 3)}.get(j, (0, 5))
        return pltpu.make_async_remote_copy(
            src_ref=pack.at[lo:hi],
            dst_ref=R.at[NBACK - i, 2 - j, lo:hi],
            send_sem=ssem.at[n],
            recv_sem=rsem.at[n],
            device_id=to(i, j),
            device_id_type=pl.DeviceIdType.MESH,
        )

    for n, (i, j) in enumerate(partners()):
        @pl.when(there(i, j))
        def _():
            copy(n, i, j).start()

    WE[...] = jnp.zeros(WE.shape, BF)
    loads[1].wait()
    for dc in range(3):
        for dt in range(3):
            for dr in range(3):
                w = ek[dt, dr, dc]
                for fo in range(2):
                    for ro in range(2):
                        k = ((fo + dt) * 4 + ro + dr) * CI
                        n = (fo * 2 + ro) * C
                        WE[dc, k:k + CI, n:n + C] = w
    loads[2].wait()
    loads[3].wait()

    def fold(s, carry):
        dt = s // 8
        r0 = pl.multiple_of((s % 8) * 32, 32)
        m = [[ubuf[dt, r, c, pl.ds(r0, 32), :].astype(F32) for c in range(3)] for r in range(3)]
        rows = [m[0], [m[0][c] + m[1][c] + m[2][c] for c in range(3)], m[2]]
        for a in range(3):
            q = rows[a]
            cols = [[q[0], q[1] + q[2]], [q[0] + q[1], q[2]]]
            for b in range(2):
                for c in range(2):
                    WU[a, b, dt, c, pl.ds(r0, 32), :] = cols[b][c].astype(BF)
        dr = dt
        for dc in range(3):
            k = [W2[t, dr, dc, pl.ds(r0, 32), :].astype(F32) for t in range(3)]
            half = 0.5 * (k[0] + k[2])
            one = 0.5 * k[1]
            WM[0, dr, dc, pl.ds(r0, 32), :] = (half + one).astype(BF)
            WM[1, dr, dc, pl.ds(r0, 32), :] = (half - one).astype(BF)
        return carry

    lax.fori_loop(0, 24, fold, 0)

    def arrived(back):
        for n, (i, j) in enumerate(partners()):
            if i == back:
                @pl.when(there(-i, -j))
                def _():
                    copy(n, i, j).wait_recv()

    row_base = me_r * height
    n_rows = nr * height
    arrived(0)
    arrived(1)
    entry(row_base, n_rows, 2, (2, 3), R, WE, V, B3)
    arrived(2)
    entry(row_base, n_rows, 1, (1,), R, WE, V, B3)
    middle(row_base, n_rows, 1, W2, WM, B3, S3, MID)
    arrived(3)
    entry(row_base, n_rows, 0, (0,), R, WE, V, B3)
    middle(row_base, n_rows, 0, W2, WM, B3, S3, MID)
    upper(WU, S3, I, CR, out)

    for n, (i, j) in enumerate(partners()):
        @pl.when(there(i, j))
        def _():
            copy(n, i, j).wait_send()


def inside(r, n_rows):
    return jnp.where((r >= 0) & (r < n_rows), 1.0, 0.0)


def window(R, fp, g):
    main, tail = [], []
    for f in range(2):
        for w in range(4):
            b, r = ROW_OF[2 * g + w]
            main.append(R[fp, b, 3 * r + f].astype(F32))
            k = 32 * (2 * r + f)
            tail.append(R[fp, b, 2].astype(F32)[:, k:k + 32])
    return jnp.concatenate([jnp.concatenate(main, axis=0).T, jnp.concatenate(tail, axis=0).T], axis=0)


FRAMES = ((0, 2, -1), (1, 2, 1), (2, 1, -1), (1, 3, -1))


def entry(row_base, n_rows, k, new, R, WE, V, B3):
    for g in range(3):
        for fp in new:
            y = window(R, fp, g)
            for d in range(3):
                z = y if d == 1 else roll_cols(y, d)
                V[d, g, fp] = z.astype(BF)
    for fo in range(2):
        acc = None
        for d in range(3):
            lhs = jnp.concatenate(
                [jnp.concatenate([V[d, g, k], V[d, g, k + 1]], axis=1) for g in range(3)], axis=0)
            p = jnp.dot(lhs, WE[d, :, fo * 512:(fo + 1) * 512], preferred_element_type=F32)
            acc = p if acc is None else acc + p
        for g in range(3):
            for ro in range(2):
                ok = inside(row_base - 2 + 2 * g + ro, n_rows)
                put3(B3, (2 * k + fo, 2 * g + ro), acc[g * W:(g + 1) * W, ro * C:(ro + 1) * C] * ok)


def middle(row_base, n_rows, p, W2, WM, B3, S3, MID):
    f0 = 2 * p
    for i in range(4):
        fa, fb, sign = FRAMES[i]
        acc = None
        for dr in range(3):
            for dc in range(3):
                u = B3[dc, f0 + fa, dr:dr + 4].reshape(4 * W, C)
                v = B3[dc, f0 + fb, dr:dr + 4].reshape(4 * W, C)
                lhs = u + v if sign > 0 else u - v
                w = W2[0, dr, dc] if i == 0 else W2[2, dr, dc] if i == 3 else WM[i - 1, dr, dc]
                q = jnp.dot(lhs, w, preferred_element_type=F32)
                acc = q if acc is None else acc + q
        if i == 0:
            MID[0] = acc
        elif i == 1:
            MID[0] = MID[0] + acc
            MID[1] = acc
        else:
            t = i - 2
            if t == 0:
                y = MID[0] + acc
                MID[1] = MID[1] - acc
            else:
                y = MID[1] - acc
            for r in range(4):
                ok = inside(row_base - 1 + r, n_rows)
                s = (B3[1, f0 + t + 2, r + 1].astype(F32) + silu(y[r * W:(r + 1) * W])) * ok
                put3(S3, (f0 + t, r), s)


def upper(WU, S3, I, CR, out):
    def prod(a, b):
        acc = None
        for dt in range(3):
            for c in range(2):
                parts = []
                for t in range(2):
                    for q in range(2):
                        x = [S3[b + c, t + dt, q + k] for k in ((0, 1), (1,), (1, 2))[a]]
                        parts.append(x[0] if a == 1 else x[0] - x[1] if a == 0 else x[1] - x[0])
                p = jnp.dot(jnp.concatenate(parts, axis=0), WU[a, b, dt, c], preferred_element_type=F32)
                acc = p if acc is None else acc + p
        return acc

    for b in range(2):
        CR[b] = prod(1, b)
    for a in range(2):
        for b in range(2):
            y = silu(prod(2 * a, b) + CR[b])
            for i in range(4):
                for h in range(2):
                    I[i, h, pl.ds(b, W, stride=2), :] = y[i * W:(i + 1) * W, h * 128:(h + 1) * 128]
        for i in range(4):
            for h in range(2):
                out[i // 2, 2 * (i % 2) + a, :, h * 128:(h + 1) * 128] = I[i, h].astype(BF)


def section(nt, nr, height, *operands):
    n = len(partners())

    def body(*refs):
        section_body(nt, nr, height, *refs)

    return pl.pallas_call(
        body,
        out_shape=jax.ShapeDtypeStruct((2, 4, 2 * W, C), BF),
        in_specs=[pl.BlockSpec(memory_space=pl.ANY)] * 4,
        out_specs=pl.BlockSpec(memory_space=pltpu.VMEM),
        scratch_shapes=[
            pltpu.VMEM((4, 5, 5, CI, 128), BF),
            pltpu.VMEM((3, 256, 1024), BF),
            pltpu.VMEM((3, 3, 3, C, C), BF),
            pltpu.VMEM((2, 3, 3, C, C), BF),
            pltpu.VMEM((3, 2, 3, 2, C, C), BF),
            pltpu.VMEM((3, 3, 4, W, 128), BF),
            pltpu.VMEM((3, 6, 6, W, C), BF),
            pltpu.VMEM((3, 4, 4, W, C), BF),
            pltpu.VMEM((4, 2, 2 * W, 128), F32),
            pltpu.VMEM((2, 4 * W, C), F32),
            pltpu.VMEM((2, 4 * W, C), F32),
            pltpu.VMEM((2, 2, CI, W), BF),
            pltpu.VMEM((3, 3, 3, CI, C), BF),
            pltpu.VMEM((3, 3, 3, C, C), BF),
            pltpu.VMEM((5, CI, 128), BF),
            pltpu.SemaphoreType.DMA((4,)),
            pltpu.SemaphoreType.DMA((n,)),
            pltpu.SemaphoreType.DMA((n,)),
        ],
        compiler_params=pltpu.CompilerParams(collective_id=0, has_side_effects=True, vmem_limit_bytes=46 * 2**20),
        name="section",
    )(*[pltpu.with_memory_space_constraint(x, pltpu.HBM) for x in operands])


def per_device(nt, nr, latent, entry_kernel, middle_kernel, upper_kernel):
    lat = jnp.transpose(latent, (0, 1, 3, 2))
    return section(nt, nr, latent.shape[1], lat, entry_kernel, upper_kernel, middle_kernel)


def solution(mesh):
    nt = mesh.shape["tm"]
    nr = mesh.shape["rows"]
    return jax.shard_map(
        lambda *a: per_device(nt, nr, *a),
        mesh=mesh,
        in_specs=(P("tm", "rows", None, None), P(), P(), P()),
        out_specs=P("tm", "rows", None, None),
        check_vma=False,
    )
```

```python
import jax
import jax.numpy as jnp
from jax import lax
from jax.experimental import pallas as pl
from jax.experimental.pallas import tpu as pltpu
from jax.sharding import PartitionSpec as P

F32 = jnp.float32
BF = jnp.bfloat16
W = 160
C = 256
CI = 16
NBACK = 3
NSIDE = 2


def roll_cols(x, d):
    n = x.shape[0]
    row = lax.broadcasted_iota(jnp.int32, x.shape, 0)
    if d == 0:
        return jnp.where(row == 0, 0.0, pltpu.roll(x, 1, 0))
    return jnp.where(row == n - 1, 0.0, pltpu.roll(x, n - 1, 0))


def silu(v):
    h = 0.5 * v
    return h + h * jnp.tanh(h)


def put3(dst, idx, x):
    for d in range(3):
        y = x if d == 1 else roll_cols(x, d)
        dst[(d,) + idx] = y.astype(BF)


def four(g):
    half = 0.5 * (g[0] + g[2])
    one = 0.5 * g[1]
    return [g[0], half + one, half - one, g[2]]


def partners():
    return [(i, j) for i in range(NBACK + 1) for j in range(-NSIDE, NSIDE + 1) if (i, j) != (0, 0)]


ROW_OF = ((0, 1), (1, 0), (1, 1), (2, 0), (2, 1), (3, 0), (3, 1), (4, 0))


def exchange_body(nt, nr, lat_h, ek_h, uk, mk, R, WE, WM, WU, lat, ek, ubuf, mbuf, pack, lsem, ssem, rsem):
    me_t = lax.axis_index("tm")
    me_r = lax.axis_index("rows")

    def there(di, dj):
        t = me_t + di
        r = me_r + dj
        return (t >= 0) & (t < nt) & (r >= 0) & (r < nr)

    def to(di, dj):
        return {"tm": me_t + di, "rows": me_r + dj}

    loads = [pltpu.make_async_copy(src, dst, lsem.at[n])
             for n, (src, dst) in enumerate(((lat_h, lat), (ek_h, ek), (uk, ubuf), (mk, mbuf)))]
    for x in loads:
        x.start()
    barrier = pltpu.get_barrier_semaphore()
    for i, j in partners():
        @pl.when(there(-i, -j))
        def _():
            pl.semaphore_signal(barrier, inc=1, device_id=to(-i, -j), device_id_type=pl.DeviceIdType.MESH)
    for i, j in partners():
        @pl.when(jnp.logical_not(there(-i, -j)))
        def _():
            R[NBACK - i, 2 - j] = jnp.zeros((5, CI, 128), BF)
    loads[0].wait()
    tails = []
    for r in range(2):
        for f in range(2):
            v = lat[f, r]
            pack[3 * r + f] = v[:, :128]
            tails.append(v[:, 128:].astype(F32))
    pack[2] = jnp.concatenate(tails, axis=1).astype(BF)
    R[NBACK, 2] = pack[...]
    ahead = jnp.minimum(nt - 1 - me_t, NBACK) + 1
    beside = jnp.minimum(me_r, NSIDE) + jnp.minimum(nr - 1 - me_r, NSIDE) + 1
    pl.semaphore_wait(barrier, ahead * beside - 1)

    def copy(n, i, j):
        lo, hi = {2: (2, 5), -2: (0, 3)}.get(j, (0, 5))
        return pltpu.make_async_remote_copy(
            src_ref=pack.at[lo:hi],
            dst_ref=R.at[NBACK - i, 2 - j, lo:hi],
            send_sem=ssem.at[n],
            recv_sem=rsem.at[n],
            device_id=to(i, j),
            device_id_type=pl.DeviceIdType.MESH,
        )

    for n, (i, j) in reversed(list(enumerate(partners()))):
        @pl.when(there(i, j))
        def _():
            copy(n, i, j).start()

    WE[...] = jnp.zeros(WE.shape, BF)
    loads[1].wait()
    for dc in range(3):
        for dt in range(3):
            for dr in range(3):
                w = ek[dt, dr, dc]
                for fo in range(2):
                    for ro in range(2):
                        k = ((fo + dt) * 4 + ro + dr) * CI
                        n = (fo * 2 + ro) * C
                        WE[dc, k:k + CI, n:n + C] = w
    loads[2].wait()
    loads[3].wait()

    def fold(s, carry):
        dt = s // 8
        r0 = pl.multiple_of((s % 8) * 32, 32)
        m = [[ubuf[dt, r, c, pl.ds(r0, 32), :].astype(F32) for c in range(3)] for r in range(3)]
        rows = [m[0], [m[0][c] + m[1][c] + m[2][c] for c in range(3)], m[2]]
        for a in range(3):
            q = rows[a]
            cols = [[q[0], q[1] + q[2]], [q[0] + q[1], q[2]]]
            for b in range(2):
                for c in range(2):
                    WU[a, b, dt, c, pl.ds(r0, 32), :] = cols[b][c].astype(BF)
        dc = dt
        k = [[mbuf[t, r, dc, pl.ds(r0, 32), :].astype(F32) for r in range(3)] for t in range(3)]
        cols = [four([k[t][r] for t in range(3)]) for r in range(3)]
        for i in range(4):
            w = four([cols[r][i] for r in range(3)])
            for j in range(4):
                WM[i, j, dc, pl.ds(r0, 32), :] = w[j].astype(BF)
        return carry

    lax.fori_loop(0, 24, fold, 0)

    for n, (i, j) in enumerate(partners()):
        @pl.when(there(i, j))
        def _():
            copy(n, i, j).wait_send()

        @pl.when(there(-i, -j))
        def _():
            copy(n, i, j).wait_recv()


def exchange(nt, nr, lat, ek, uk, mk):
    vm = pl.BlockSpec(memory_space=pltpu.VMEM)
    hbm = pl.BlockSpec(memory_space=pl.ANY)
    n = len(partners())

    def body(*refs):
        exchange_body(nt, nr, *refs)

    return pl.pallas_call(
        body,
        out_shape=(
            jax.ShapeDtypeStruct((4, 5, 5, CI, 128), BF),
            jax.ShapeDtypeStruct((3, 256, 1024), BF),
            jax.ShapeDtypeStruct((4, 4, 3, C, C), BF),
            jax.ShapeDtypeStruct((3, 2, 3, 2, C, C), BF),
        ),
        in_specs=[hbm] * 4,
        out_specs=(vm,) * 4,
        scratch_shapes=[
            pltpu.VMEM((2, 2, CI, W), BF),
            pltpu.VMEM((3, 3, 3, CI, C), BF),
            pltpu.VMEM((3, 3, 3, C, C), BF),
            pltpu.VMEM((3, 3, 3, C, C), BF),
            pltpu.VMEM((5, CI, 128), BF),
            pltpu.SemaphoreType.DMA((4,)),
            pltpu.SemaphoreType.DMA((n,)),
            pltpu.SemaphoreType.DMA((n,)),
        ],
        compiler_params=pltpu.CompilerParams(collective_id=0, has_side_effects=True, vmem_limit_bytes=16 * 2**20),
        name="exchange",
    )(*[pltpu.with_memory_space_constraint(x, pltpu.HBM) for x in (lat, ek, uk, mk)])


def window(R, fp, g):
    main, tail = [], []
    for f in range(2):
        for w in range(4):
            b, r = ROW_OF[2 * g + w]
            main.append(R[fp, b, 3 * r + f].astype(F32))
            k = 32 * (2 * r + f)
            tail.append(R[fp, b, 2].astype(F32)[:, k:k + 32])
    return jnp.concatenate([jnp.concatenate(main, axis=0).T, jnp.concatenate(tail, axis=0).T], axis=0)


PAIRS = ((0, 2, -1), (1, 2, 1), (2, 1, -1), (1, 3, -1))


def decode_body(n_rows, height, R, WE, WM, WU, out_h, out, V, B3, S3, I, CR, MID, Y, osem):
    row_base = lax.axis_index("rows") * height

    def inside(r):
        return jnp.where((r >= 0) & (r < n_rows), 1.0, 0.0)

    for g in range(3):
        for fp in range(4):
            y = window(R, fp, g)
            for d in range(3):
                z = y if d == 1 else roll_cols(y, d)
                V[d, g, fp] = z.astype(BF)
    for g in range(3):
        for fo in range(2):
            acc = None
            for d in range(3):
                lhs = jnp.concatenate(
                    [jnp.concatenate([V[d, g, k], V[d, g, k + 1]], axis=1) for k in range(3)], axis=0)
                p = jnp.dot(lhs, WE[d, :, fo * 512:(fo + 1) * 512], preferred_element_type=F32)
                acc = p if acc is None else acc + p
            for ro in range(2):
                ok = inside(row_base - 2 + 2 * g + ro)
                for k in range(3):
                    put3(B3, (2 * k + fo, 2 * g + ro), acc[k * W:(k + 1) * W, ro * C:(ro + 1) * C] * ok)

    def product(i, j):
        fa, fb, fs = PAIRS[i]
        ra, rb, rs = PAIRS[j]
        acc = None
        for dc in range(3):
            parts = []
            for p in range(2):
                for q in range(2):
                    x = [B3[dc, 2 * p + f, 2 * q + r] for f in (fa, fb) for r in (ra, rb)]
                    u, v = (x[0] + x[1], x[2] + x[3]) if rs > 0 else (x[0] - x[1], x[2] - x[3])
                    parts.append(u + v if fs > 0 else u - v)
            z = jnp.dot(jnp.concatenate(parts, axis=0), WM[i, j, dc], preferred_element_type=F32)
            acc = z if acc is None else acc + z
        return acc

    def finish(t, h, y):
        for p in range(2):
            for q in range(2):
                r = 2 * q + h
                m = (2 * p + q) * W
                s = (B3[1, 2 * p + t + 2, r + 1].astype(F32) + silu(y[m:m + W])) * inside(row_base - 1 + r)
                put3(S3, (2 * p + t, r), s)

    for i in range(4):
        MID[0] = product(i, 0)
        x = product(i, 1)
        MID[0] = MID[0] + x
        MID[1] = x
        for h in range(2):
            if h == 0:
                x = product(i, 2)
                z = MID[0] + x
                MID[1] = MID[1] - x
            else:
                z = MID[1] - product(i, 3)
            if i == 0:
                Y[0, h] = z
            elif i == 1:
                Y[0, h] = Y[0, h] + z
                Y[1, h] = z
            elif i == 2:
                finish(0, h, Y[0, h] + z)
                Y[1, h] = Y[1, h] - z
            else:
                finish(1, h, Y[1, h] - z)

    def prod(a, b):
        acc = None
        for dt in (2, 1, 0):
            for c in range(2):
                parts = []
                for t in range(2):
                    for q in range(2):
                        x = [S3[b + c, t + dt, q + k] for k in ((0, 1), (1,), (1, 2))[a]]
                        parts.append(x[0] if a == 1 else x[0] - x[1] if a == 0 else x[1] - x[0])
                p = jnp.dot(jnp.concatenate(parts, axis=0), WU[a, b, dt, c], preferred_element_type=F32)
                acc = p if acc is None else acc + p
        return acc

    def store(a, i):
        at = (i // 2, 2 * (i % 2) + a)
        return pltpu.make_async_copy(out.at[at], out_h.at[at], osem.at[4 * a + i])

    for b in range(2):
        CR[b] = prod(1, b)
    for a in range(2):
        for b in range(2):
            y = silu(prod(2 * a, b) + CR[b])
            for i in range(4):
                for h in range(2):
                    I[i, h, pl.ds(b, W, stride=2), :] = y[i * W:(i + 1) * W, h * 128:(h + 1) * 128]
        for i in range(4):
            for h in range(2):
                out[i // 2, 2 * (i % 2) + a, :, h * 128:(h + 1) * 128] = I[i, h].astype(BF)
            store(a, i).start()
    for a in range(2):
        for i in range(4):
            store(a, i).wait()


def decode(n_rows, height, *operands):
    vm = pl.BlockSpec(memory_space=pltpu.VMEM)

    def body(*refs):
        decode_body(n_rows, height, *refs)

    return pl.pallas_call(
        body,
        out_shape=jax.ShapeDtypeStruct((2, 4, 2 * W, C), BF),
        in_specs=[vm] * len(operands),
        out_specs=pl.BlockSpec(memory_space=pl.ANY),
        scratch_shapes=[
            pltpu.VMEM((2, 4, 2 * W, C), BF),
            pltpu.VMEM((3, 3, 4, W, 128), BF),
            pltpu.VMEM((3, 6, 6, W, C), BF),
            pltpu.VMEM((3, 4, 4, W, C), BF),
            pltpu.VMEM((4, 2, 2 * W, 128), F32),
            pltpu.VMEM((2, 4 * W, C), F32),
            pltpu.VMEM((2, 4 * W, C), F32),
            pltpu.VMEM((2, 2, 4 * W, C), F32),
            pltpu.SemaphoreType.DMA((8,)),
        ],
        compiler_params=pltpu.CompilerParams(vmem_limit_bytes=32 * 2**20),
        name="decode",
    )(*operands)


def per_device(nt, nr, latent, entry_kernel, middle_kernel, upper_kernel):
    height = latent.shape[1]
    lat = jnp.transpose(latent, (0, 1, 3, 2))
    return decode(height * nr, height, *exchange(nt, nr, lat, entry_kernel, upper_kernel, middle_kernel))


def solution(mesh):
    nt = mesh.shape["tm"]
    nr = mesh.shape["rows"]
    return jax.shard_map(
        lambda *a: per_device(nt, nr, *a),
        mesh=mesh,
        in_specs=(P("tm", "rows", None, None), P(), P(), P()),
        out_specs=P("tm", "rows", None, None),
        check_vma=False,
    )
```

```python
import jax
import jax.numpy as jnp
from jax import lax
from jax.experimental import pallas as pl
from jax.experimental.pallas import tpu as pltpu
from jax.sharding import PartitionSpec as P

F32 = jnp.float32
BF = jnp.bfloat16
W = 160
C = 256
CI = 16
NBACK = 3
NSIDE = 2
ORDER = (2, 1, 3, 0)


def roll_cols(x, d):
    n = x.shape[0]
    row = lax.broadcasted_iota(jnp.int32, x.shape, 0)
    if d == 0:
        return jnp.where(row == 0, 0.0, pltpu.roll(x, 1, 0))
    return jnp.where(row == n - 1, 0.0, pltpu.roll(x, n - 1, 0))


def silu(v):
    h = 0.5 * v
    return h + h * jnp.tanh(h)


def put3(dst, idx, x):
    for d in range(3):
        y = x if d == 1 else roll_cols(x, d)
        dst[(d,) + idx] = y.astype(BF)


def four(g):
    half = 0.5 * (g[0] + g[2])
    one = 0.5 * g[1]
    return [g[0], half + one, half - one, g[2]]


def partners():
    return [(i, j) for i in range(NBACK + 1) for j in range(-NSIDE, NSIDE + 1) if (i, j) != (0, 0)]


ROW_OF = ((0, 1), (1, 0), (1, 1), (2, 0), (2, 1), (3, 0), (3, 1), (4, 0))


def exchange_body(nt, nr, lat_h, ek_h, uk, mk, R, WE, WM, WU, lat, ek, ubuf, mbuf, pack, lsem, ssem, rsem, fsem):
    me_t = lax.axis_index("tm")
    me_r = lax.axis_index("rows")

    def there(di, dj):
        t = me_t + di
        r = me_r + dj
        return (t >= 0) & (t < nt) & (r >= 0) & (r < nr)

    def to(di, dj):
        return {"tm": me_t + di, "rows": me_r + dj}

    even = lax.rem(me_t, 2) == 0
    odd = lax.rem(me_t, 2) == 1

    def sends(i, j):
        return there(i, j) & even if i == 2 else there(i, j) & odd if i == 3 else there(i, j)

    def gets(i, j):
        return there(-i, -j) & even if i >= 2 else there(-i, -j)

    loads = [pltpu.make_async_copy(src, dst, lsem.at[n])
             for n, (src, dst) in enumerate(((lat_h, lat), (ek_h, ek), (uk, ubuf), (mk, mbuf)))]
    for x in loads:
        x.start()
    barrier = pltpu.get_barrier_semaphore()
    for i, j in partners():
        @pl.when(gets(i, j))
        def _():
            pl.semaphore_signal(barrier, inc=1, device_id=to(-i, -j), device_id_type=pl.DeviceIdType.MESH)
    for i, j in partners():
        @pl.when(jnp.logical_not(there(-i, -j)))
        def _():
            R[NBACK - i, 2 - j] = jnp.zeros((5, CI, 128), BF)
    loads[0].wait()
    tails = []
    for r in range(2):
        for f in range(2):
            v = lat[f, r]
            pack[3 * r + f] = v[:, :128]
            tails.append(v[:, 128:].astype(F32))
    pack[2] = jnp.concatenate(tails, axis=1).astype(BF)
    R[NBACK, 2] = pack[...]
    far = jnp.where(even, 2, 3)
    ahead = 1 + jnp.where(me_t + 1 < nt, 1, 0) + jnp.where(me_t + far < nt, 1, 0)
    beside = jnp.minimum(me_r, NSIDE) + jnp.minimum(nr - 1 - me_r, NSIDE) + 1
    pl.semaphore_wait(barrier, ahead * beside - 1)

    def copy(n, i, j):
        lo, hi = {2: (2, 5), -2: (0, 3)}.get(j, (0, 5))
        return pltpu.make_async_remote_copy(
            src_ref=pack.at[lo:hi],
            dst_ref=R.at[NBACK - i, 2 - j, lo:hi],
            send_sem=ssem.at[n],
            recv_sem=rsem.at[n],
            device_id=to(i, j),
            device_id_type=pl.DeviceIdType.MESH,
        )

    def forward(n, i, j):
        lo, hi = {2: (2, 5), -2: (0, 3)}.get(j, (0, 5))
        return pltpu.make_async_remote_copy(
            src_ref=R.at[NBACK - i, 2 - j, lo:hi],
            dst_ref=R.at[NBACK - i - 1, 2 - j, lo:hi],
            send_sem=fsem.at[n],
            recv_sem=rsem.at[index[i + 1, j]],
            device_id=to(1, 0),
            device_id_type=pl.DeviceIdType.MESH,
        )

    index = {ij: n for n, ij in enumerate(partners())}
    for i in ORDER:
        for j in range(-NSIDE, NSIDE + 1):
            if (i, j) in index:
                @pl.when(sends(i, j))
                def _():
                    copy(index[i, j], i, j).start()

    WE[...] = jnp.zeros(WE.shape, BF)
    loads[1].wait()
    for dc in range(3):
        for dt in range(3):
            for dr in range(3):
                w = ek[dt, dr, dc]
                for fo in range(2):
                    for ro in range(2):
                        k = ((fo + dt) * 4 + ro + dr) * CI
                        n = (fo * 2 + ro) * C
                        WE[dc, k:k + CI, n:n + C] = w
    loads[2].wait()
    loads[3].wait()

    def fold(s, carry):
        dt = s // 8
        r0 = pl.multiple_of((s % 8) * 32, 32)
        m = [[ubuf[dt, r, c, pl.ds(r0, 32), :].astype(F32) for c in range(3)] for r in range(3)]
        rows = [m[0], [m[0][c] + m[1][c] + m[2][c] for c in range(3)], m[2]]
        for a in range(3):
            q = rows[a]
            cols = [[q[0], q[1] + q[2]], [q[0] + q[1], q[2]]]
            for b in range(2):
                for c in range(2):
                    WU[a, b, dt, c, pl.ds(r0, 32), :] = cols[b][c].astype(BF)
        dc = dt
        k = [[mbuf[t, r, dc, pl.ds(r0, 32), :].astype(F32) for r in range(3)] for t in range(3)]
        cols = [four([k[t][r] for t in range(3)]) for r in range(3)]
        for i in range(4):
            w = four([cols[r][i] for r in range(3)])
            for j in range(4):
                WM[i, j, dc, pl.ds(r0, 32), :] = w[j].astype(BF)
        return carry

    lax.fori_loop(0, 24, fold, 0)

    relayed = [(i, j) for i in (1, 2) for j in range(-NSIDE, NSIDE + 1)]
    for i, j in relayed:
        @pl.when(there(-i, -j) & even)
        def _():
            copy(index[i, j], i, j).wait_recv()

        @pl.when(there(-i, -j) & even & there(1, 0))
        def _():
            forward(index[i, j], i, j).start()
    for n, (i, j) in enumerate(partners()):
        @pl.when(there(-i, -j) & odd if (i, j) in relayed else there(-i, -j))
        def _():
            copy(n, i, j).wait_recv()
    for n, (i, j) in enumerate(partners()):
        @pl.when(sends(i, j))
        def _():
            copy(n, i, j).wait_send()
    for i, j in relayed:
        @pl.when(there(-i, -j) & even & there(1, 0))
        def _():
            forward(index[i, j], i, j).wait_send()


def exchange(nt, nr, lat, ek, uk, mk):
    vm = pl.BlockSpec(memory_space=pltpu.VMEM)
    hbm = pl.BlockSpec(memory_space=pl.ANY)
    n = len(partners())

    def body(*refs):
        exchange_body(nt, nr, *refs)

    return pl.pallas_call(
        body,
        out_shape=(
            jax.ShapeDtypeStruct((4, 5, 5, CI, 128), BF),
            jax.ShapeDtypeStruct((3, 256, 1024), BF),
            jax.ShapeDtypeStruct((4, 4, 3, C, C), BF),
            jax.ShapeDtypeStruct((3, 2, 3, 2, C, C), BF),
        ),
        in_specs=[hbm] * 4,
        out_specs=(vm,) * 4,
        scratch_shapes=[
            pltpu.VMEM((2, 2, CI, W), BF),
            pltpu.VMEM((3, 3, 3, CI, C), BF),
            pltpu.VMEM((3, 3, 3, C, C), BF),
            pltpu.VMEM((3, 3, 3, C, C), BF),
            pltpu.VMEM((5, CI, 128), BF),
            pltpu.SemaphoreType.DMA((4,)),
            pltpu.SemaphoreType.DMA((n,)),
            pltpu.SemaphoreType.DMA((n,)),
            pltpu.SemaphoreType.DMA((n,)),
        ],
        compiler_params=pltpu.CompilerParams(collective_id=0, has_side_effects=True, vmem_limit_bytes=16 * 2**20),
        name="exchange",
    )(*[pltpu.with_memory_space_constraint(x, pltpu.HBM) for x in (lat, ek, uk, mk)])


def window(R, fp, g):
    main, tail = [], []
    for f in range(2):
        for w in range(4):
            b, r = ROW_OF[2 * g + w]
            main.append(R[fp, b, 3 * r + f].astype(F32))
            k = 32 * (2 * r + f)
            tail.append(R[fp, b, 2].astype(F32)[:, k:k + 32])
    return jnp.concatenate([jnp.concatenate(main, axis=0).T, jnp.concatenate(tail, axis=0).T], axis=0)


PAIRS = ((0, 2, -1), (1, 2, 1), (2, 1, -1), (1, 3, -1))


def decode_body(n_rows, height, R, WE, WM, WU, out_h, out, V, B3, S3, I, CR, MID, Y, osem):
    row_base = lax.axis_index("rows") * height

    def inside(r):
        return jnp.where((r >= 0) & (r < n_rows), 1.0, 0.0)

    for g in range(3):
        for fp in range(4):
            y = window(R, fp, g)
            for d in range(3):
                z = y if d == 1 else roll_cols(y, d)
                V[d, g, fp] = z.astype(BF)
    for g in range(3):
        for fo in range(2):
            acc = None
            for d in range(3):
                lhs = jnp.concatenate(
                    [jnp.concatenate([V[d, g, k], V[d, g, k + 1]], axis=1) for k in range(3)], axis=0)
                p = jnp.dot(lhs, WE[d, :, fo * 512:(fo + 1) * 512], preferred_element_type=F32)
                acc = p if acc is None else acc + p
            for ro in range(2):
                ok = inside(row_base - 2 + 2 * g + ro)
                for k in range(3):
                    put3(B3, (2 * k + fo, 2 * g + ro), acc[k * W:(k + 1) * W, ro * C:(ro + 1) * C] * ok)

    def product(i, j):
        fa, fb, fs = PAIRS[i]
        ra, rb, rs = PAIRS[j]
        acc = None
        for dc in range(3):
            parts = []
            for p in range(2):
                for q in range(2):
                    x = [B3[dc, 2 * p + f, 2 * q + r] for f in (fa, fb) for r in (ra, rb)]
                    u, v = (x[0] + x[1], x[2] + x[3]) if rs > 0 else (x[0] - x[1], x[2] - x[3])
                    parts.append(u + v if fs > 0 else u - v)
            z = jnp.dot(jnp.concatenate(parts, axis=0), WM[i, j, dc], preferred_element_type=F32)
            acc = z if acc is None else acc + z
        return acc

    def finish(t, h, y):
        for p in range(2):
            for q in range(2):
                r = 2 * q + h
                m = (2 * p + q) * W
                s = (B3[1, 2 * p + t + 2, r + 1].astype(F32) + silu(y[m:m + W])) * inside(row_base - 1 + r)
                put3(S3, (2 * p + t, r), s)

    for i in range(4):
        MID[0] = product(i, 0)
        x = product(i, 1)
        MID[0] = MID[0] + x
        MID[1] = x
        for h in range(2):
            if h == 0:
                x = product(i, 2)
                z = MID[0] + x
                MID[1] = MID[1] - x
            else:
                z = MID[1] - product(i, 3)
            if i == 0:
                Y[0, h] = z
            elif i == 1:
                Y[0, h] = Y[0, h] + z
                Y[1, h] = z
            elif i == 2:
                finish(0, h, Y[0, h] + z)
                Y[1, h] = Y[1, h] - z
            else:
                finish(1, h, Y[1, h] - z)

    def prod(a, b):
        acc = None
        for dt in (2, 1, 0):
            for c in range(2):
                parts = []
                for t in range(2):
                    for q in range(2):
                        x = [S3[b + c, t + dt, q + k] for k in ((0, 1), (1,), (1, 2))[a]]
                        parts.append(x[0] if a == 1 else x[0] - x[1] if a == 0 else x[1] - x[0])
                p = jnp.dot(jnp.concatenate(parts, axis=0), WU[a, b, dt, c], preferred_element_type=F32)
                acc = p if acc is None else acc + p
        return acc

    def store(a, i):
        at = (i // 2, 2 * (i % 2) + a)
        return pltpu.make_async_copy(out.at[at], out_h.at[at], osem.at[4 * a + i])

    for b in range(2):
        CR[b] = prod(1, b)
    for a in range(2):
        for b in range(2):
            y = silu(prod(2 * a, b) + CR[b])
            for i in range(4):
                for h in range(2):
                    I[i, h, pl.ds(b, W, stride=2), :] = y[i * W:(i + 1) * W, h * 128:(h + 1) * 128]
        for i in range(4):
            for h in range(2):
                out[i // 2, 2 * (i % 2) + a, :, h * 128:(h + 1) * 128] = I[i, h].astype(BF)
            store(a, i).start()
    for a in range(2):
        for i in range(4):
            store(a, i).wait()


def decode(n_rows, height, *operands):
    vm = pl.BlockSpec(memory_space=pltpu.VMEM)

    def body(*refs):
        decode_body(n_rows, height, *refs)

    return pl.pallas_call(
        body,
        out_shape=jax.ShapeDtypeStruct((2, 4, 2 * W, C), BF),
        in_specs=[vm] * len(operands),
        out_specs=pl.BlockSpec(memory_space=pl.ANY),
        scratch_shapes=[
            pltpu.VMEM((2, 4, 2 * W, C), BF),
            pltpu.VMEM((3, 3, 4, W, 128), BF),
            pltpu.VMEM((3, 6, 6, W, C), BF),
            pltpu.VMEM((3, 4, 4, W, C), BF),
            pltpu.VMEM((4, 2, 2 * W, 128), F32),
            pltpu.VMEM((2, 4 * W, C), F32),
            pltpu.VMEM((2, 4 * W, C), F32),
            pltpu.VMEM((2, 2, 4 * W, C), F32),
            pltpu.SemaphoreType.DMA((8,)),
        ],
        compiler_params=pltpu.CompilerParams(vmem_limit_bytes=32 * 2**20),
        name="decode",
    )(*operands)


def per_device(nt, nr, latent, entry_kernel, middle_kernel, upper_kernel):
    height = latent.shape[1]
    lat = jnp.transpose(latent, (0, 1, 3, 2))
    return decode(height * nr, height, *exchange(nt, nr, lat, entry_kernel, upper_kernel, middle_kernel))


def solution(mesh):
    nt = mesh.shape["tm"]
    nr = mesh.shape["rows"]
    return jax.shard_map(
        lambda *a: per_device(nt, nr, *a),
        mesh=mesh,
        in_specs=(P("tm", "rows", None, None), P(), P(), P()),
        out_specs=P("tm", "rows", None, None),
        check_vma=False,
    )
```

```python
import jax
import jax.numpy as jnp
from jax import lax
from jax.experimental import pallas as pl
from jax.experimental.pallas import tpu as pltpu
from jax.sharding import PartitionSpec as P

F32 = jnp.float32
BF = jnp.bfloat16
W = 160
C = 256
CI = 16
NBACK = 3
NSIDE = 2
ORDER = (2, 1, 0)


def roll_cols(x, d):
    n = x.shape[0]
    row = lax.broadcasted_iota(jnp.int32, x.shape, 0)
    if d == 0:
        return jnp.where(row == 0, 0.0, pltpu.roll(x, 1, 0))
    return jnp.where(row == n - 1, 0.0, pltpu.roll(x, n - 1, 0))


def silu(v):
    h = 0.5 * v
    return h + h * jnp.tanh(h)


def put3(dst, idx, x):
    for d in range(3):
        y = x if d == 1 else roll_cols(x, d)
        dst[(d,) + idx] = y.astype(BF)


def four(g):
    half = 0.5 * (g[0] + g[2])
    one = 0.5 * g[1]
    return [g[0], half + one, half - one, g[2]]


def partners():
    return [(i, j) for i in range(NBACK + 1) for j in range(-NSIDE, NSIDE + 1) if (i, j) != (0, 0)]


ROW_OF = ((0, 1), (1, 0), (1, 1), (2, 0), (2, 1), (3, 0), (3, 1), (4, 0))


def exchange_body(nt, nr, lat_h, ek_h, uk, mk, R, WE, WM, WU, lat, ek, ubuf, mbuf, pack, lsem, ssem, rsem, fsem):
    me_t = lax.axis_index("tm")
    me_r = lax.axis_index("rows")

    def there(di, dj):
        t = me_t + di
        r = me_r + dj
        return (t >= 0) & (t < nt) & (r >= 0) & (r < nr)

    def to(di, dj):
        return {"tm": me_t + di, "rows": me_r + dj}

    even = lax.rem(me_t, 2) == 0
    odd = lax.rem(me_t, 2) == 1

    def sends(i, j):
        return there(i, j) & even if i == 2 else there(i, j)

    def gets(i, j):
        return there(-i, -j) & even if i == 2 else there(-i, -j)

    loads = [pltpu.make_async_copy(src, dst, lsem.at[n])
             for n, (src, dst) in enumerate(((lat_h, lat), (ek_h, ek), (uk, ubuf), (mk, mbuf)))]
    for x in loads:
        x.start()
    barrier = pltpu.get_barrier_semaphore()
    for i, j in partners():
        if i < NBACK:
            @pl.when(gets(i, j))
            def _():
                pl.semaphore_signal(barrier, inc=1, device_id=to(-i, -j), device_id_type=pl.DeviceIdType.MESH)
    for i, j in partners():
        @pl.when(jnp.logical_not(there(-i, -j)))
        def _():
            R[NBACK - i, 2 - j] = jnp.zeros((5, CI, 128), BF)
    loads[0].wait()
    tails = []
    for r in range(2):
        for f in range(2):
            v = lat[f, r]
            pack[3 * r + f] = v[:, :128]
            tails.append(v[:, 128:].astype(F32))
    pack[2] = jnp.concatenate(tails, axis=1).astype(BF)
    R[NBACK, 2] = pack[...]
    ahead = 1 + jnp.where(me_t + 1 < nt, 1, 0) + jnp.where(even & (me_t + 2 < nt), 1, 0)
    beside = jnp.minimum(me_r, NSIDE) + jnp.minimum(nr - 1 - me_r, NSIDE) + 1
    pl.semaphore_wait(barrier, ahead * beside - 1)

    def copy(n, i, j):
        lo, hi = {2: (2, 5), -2: (0, 3)}.get(j, (0, 5))
        return pltpu.make_async_remote_copy(
            src_ref=pack.at[lo:hi],
            dst_ref=R.at[NBACK - i, 2 - j, lo:hi],
            send_sem=ssem.at[n],
            recv_sem=rsem.at[n],
            device_id=to(i, j),
            device_id_type=pl.DeviceIdType.MESH,
        )

    def forward(i, j, step):
        lo, hi = {2: (2, 5), -2: (0, 3)}.get(j, (0, 5))
        return pltpu.make_async_remote_copy(
            src_ref=R.at[NBACK - i, 2 - j, lo:hi],
            dst_ref=R.at[NBACK - i - step, 2 - j, lo:hi],
            send_sem=fsem.at[step - 1, index[i, j]],
            recv_sem=rsem.at[index[i + step, j]],
            device_id=to(step, 0),
            device_id_type=pl.DeviceIdType.MESH,
        )

    index = {ij: n for n, ij in enumerate(partners())}
    for i in ORDER:
        for j in range(-NSIDE, NSIDE + 1):
            if (i, j) in index:
                @pl.when(sends(i, j))
                def _():
                    copy(index[i, j], i, j).start()

    WE[...] = jnp.zeros(WE.shape, BF)
    loads[1].wait()
    for dc in range(3):
        for dt in range(3):
            for dr in range(3):
                w = ek[dt, dr, dc]
                for fo in range(2):
                    for ro in range(2):
                        k = ((fo + dt) * 4 + ro + dr) * CI
                        n = (fo * 2 + ro) * C
                        WE[dc, k:k + CI, n:n + C] = w
    loads[2].wait()
    loads[3].wait()

    def fold(s, carry):
        dt = s // 8
        r0 = pl.multiple_of((s % 8) * 32, 32)
        m = [[ubuf[dt, r, c, pl.ds(r0, 32), :].astype(F32) for c in range(3)] for r in range(3)]
        rows = [m[0], [m[0][c] + m[1][c] + m[2][c] for c in range(3)], m[2]]
        for a in range(3):
            q = rows[a]
            cols = [[q[0], q[1] + q[2]], [q[0] + q[1], q[2]]]
            for b in range(2):
                for c in range(2):
                    WU[a, b, dt, c, pl.ds(r0, 32), :] = cols[b][c].astype(BF)
        dc = dt
        k = [[mbuf[t, r, dc, pl.ds(r0, 32), :].astype(F32) for r in range(3)] for t in range(3)]
        cols = [four([k[t][r] for t in range(3)]) for r in range(3)]
        for i in range(4):
            w = four([cols[r][i] for r in range(3)])
            for j in range(4):
                WM[i, j, dc, pl.ds(r0, 32), :] = w[j].astype(BF)
        return carry

    lax.fori_loop(0, 24, fold, 0)

    relayed = [(i, j) for i in (1, 2) for j in range(-NSIDE, NSIDE + 1)]
    for i, j in relayed:
        @pl.when(there(-i, -j) & even)
        def _():
            copy(index[i, j], i, j).wait_recv()

        for step in (2, 1)[i - 1:]:
            @pl.when(there(-i, -j) & even & there(step, 0))
            def _():
                forward(i, j, step).start()
    for n, (i, j) in enumerate(partners()):
        @pl.when(there(-i, -j) & odd if (i, j) in relayed else there(-i, -j))
        def _():
            copy(n, i, j).wait_recv()
    for n, (i, j) in enumerate(partners()):
        if i < NBACK:
            @pl.when(sends(i, j))
            def _():
                copy(n, i, j).wait_send()
    for i, j in relayed:
        for step in (2, 1)[i - 1:]:
            @pl.when(there(-i, -j) & even & there(step, 0))
            def _():
                forward(i, j, step).wait_send()


def exchange(nt, nr, lat, ek, uk, mk):
    vm = pl.BlockSpec(memory_space=pltpu.VMEM)
    hbm = pl.BlockSpec(memory_space=pl.ANY)
    n = len(partners())

    def body(*refs):
        exchange_body(nt, nr, *refs)

    return pl.pallas_call(
        body,
        out_shape=(
            jax.ShapeDtypeStruct((4, 5, 5, CI, 128), BF),
            jax.ShapeDtypeStruct((3, 256, 1024), BF),
            jax.ShapeDtypeStruct((4, 4, 3, C, C), BF),
            jax.ShapeDtypeStruct((3, 2, 3, 2, C, C), BF),
        ),
        in_specs=[hbm] * 4,
        out_specs=(vm,) * 4,
        scratch_shapes=[
            pltpu.VMEM((2, 2, CI, W), BF),
            pltpu.VMEM((3, 3, 3, CI, C), BF),
            pltpu.VMEM((3, 3, 3, C, C), BF),
            pltpu.VMEM((3, 3, 3, C, C), BF),
            pltpu.VMEM((5, CI, 128), BF),
            pltpu.SemaphoreType.DMA((4,)),
            pltpu.SemaphoreType.DMA((n,)),
            pltpu.SemaphoreType.DMA((n,)),
            pltpu.SemaphoreType.DMA((2, n)),
        ],
        compiler_params=pltpu.CompilerParams(collective_id=0, has_side_effects=True, vmem_limit_bytes=16 * 2**20),
        name="exchange",
    )(*[pltpu.with_memory_space_constraint(x, pltpu.HBM) for x in (lat, ek, uk, mk)])


def window(R, fp, g):
    main, tail = [], []
    for f in range(2):
        for w in range(4):
            b, r = ROW_OF[2 * g + w]
            main.append(R[fp, b, 3 * r + f].astype(F32))
            k = 32 * (2 * r + f)
            tail.append(R[fp, b, 2].astype(F32)[:, k:k + 32])
    return jnp.concatenate([jnp.concatenate(main, axis=0).T, jnp.concatenate(tail, axis=0).T], axis=0)


PAIRS = ((0, 2, -1), (1, 2, 1), (2, 1, -1), (1, 3, -1))


def decode_body(n_rows, height, R, WE, WM, WU, out_h, out, V, B3, S3, I, CR, MID, Y, osem):
    row_base = lax.axis_index("rows") * height

    def inside(r):
        return jnp.where((r >= 0) & (r < n_rows), 1.0, 0.0)

    for g in range(3):
        for fp in range(4):
            y = window(R, fp, g)
            for d in range(3):
                z = y if d == 1 else roll_cols(y, d)
                V[d, g, fp] = z.astype(BF)
    for g in range(3):
        for fo in range(2):
            acc = None
            for d in range(3):
                lhs = jnp.concatenate(
                    [jnp.concatenate([V[d, g, k], V[d, g, k + 1]], axis=1) for k in range(3)], axis=0)
                p = jnp.dot(lhs, WE[d, :, fo * 512:(fo + 1) * 512], preferred_element_type=F32)
                acc = p if acc is None else acc + p
            for ro in range(2):
                ok = inside(row_base - 2 + 2 * g + ro)
                for k in range(3):
                    put3(B3, (2 * k + fo, 2 * g + ro), acc[k * W:(k + 1) * W, ro * C:(ro + 1) * C] * ok)

    def product(i, j):
        fa, fb, fs = PAIRS[i]
        ra, rb, rs = PAIRS[j]
        acc = None
        for dc in range(3):
            parts = []
            for p in range(2):
                for q in range(2):
                    x = [B3[dc, 2 * p + f, 2 * q + r] for f in (fa, fb) for r in (ra, rb)]
                    u, v = (x[0] + x[1], x[2] + x[3]) if rs > 0 else (x[0] - x[1], x[2] - x[3])
                    parts.append(u + v if fs > 0 else u - v)
            z = jnp.dot(jnp.concatenate(parts, axis=0), WM[i, j, dc], preferred_element_type=F32)
            acc = z if acc is None else acc + z
        return acc

    def finish(t, h, y):
        for p in range(2):
            for q in range(2):
                r = 2 * q + h
                m = (2 * p + q) * W
                s = (B3[1, 2 * p + t + 2, r + 1].astype(F32) + silu(y[m:m + W])) * inside(row_base - 1 + r)
                put3(S3, (2 * p + t, r), s)

    for i in range(4):
        MID[0] = product(i, 0)
        x = product(i, 1)
        MID[0] = MID[0] + x
        MID[1] = x
        for h in range(2):
            if h == 0:
                x = product(i, 2)
                z = MID[0] + x
                MID[1] = MID[1] - x
            else:
                z = MID[1] - product(i, 3)
            if i == 0:
                Y[0, h] = z
            elif i == 1:
                Y[0, h] = Y[0, h] + z
                Y[1, h] = z
            elif i == 2:
                finish(0, h, Y[0, h] + z)
                Y[1, h] = Y[1, h] - z
            else:
                finish(1, h, Y[1, h] - z)

    def prod(a, b, frames=(0, 1)):
        acc = None
        for dt in (2, 1, 0):
            for c in range(2):
                parts = []
                for t in frames:
                    for q in range(2):
                        x = [S3[b + c, t + dt, q + k] for k in ((0, 1), (1,), (1, 2))[a]]
                        parts.append(x[0] if a == 1 else x[0] - x[1] if a == 0 else x[1] - x[0])
                p = jnp.dot(jnp.concatenate(parts, axis=0), WU[a, b, dt, c], preferred_element_type=F32)
                acc = p if acc is None else acc + p
        return acc

    def store(a, i):
        at = (i // 2, 2 * (i % 2) + a)
        return pltpu.make_async_copy(out.at[at], out_h.at[at], osem.at[4 * a + i])

    for b in range(2):
        CR[b] = prod(1, b)
    for a, frames in ((0, (0, 1)), (1, (0,)), (1, (1,))):
        cells = [2 * t + q for t in frames for q in range(2)]
        lo = cells[0] * W
        hi = lo + len(cells) * W
        for b in range(2):
            y = silu(prod(2 * a, b, frames) + CR[b, lo:hi])
            for i in cells:
                for h in range(2):
                    I[i, h, pl.ds(b, W, stride=2), :] = y[i * W - lo:(i + 1) * W - lo, h * 128:(h + 1) * 128]
        for i in cells:
            for h in range(2):
                out[i // 2, 2 * (i % 2) + a, :, h * 128:(h + 1) * 128] = I[i, h].astype(BF)
            store(a, i).start()
    for a in range(2):
        for i in range(4):
            store(a, i).wait()


def decode(n_rows, height, *operands):
    vm = pl.BlockSpec(memory_space=pltpu.VMEM)

    def body(*refs):
        decode_body(n_rows, height, *refs)

    return pl.pallas_call(
        body,
        out_shape=jax.ShapeDtypeStruct((2, 4, 2 * W, C), BF),
        in_specs=[vm] * len(operands),
        out_specs=pl.BlockSpec(memory_space=pl.ANY),
        scratch_shapes=[
            pltpu.VMEM((2, 4, 2 * W, C), BF),
            pltpu.VMEM((3, 3, 4, W, 128), BF),
            pltpu.VMEM((3, 6, 6, W, C), BF),
            pltpu.VMEM((3, 4, 4, W, C), BF),
            pltpu.VMEM((4, 2, 2 * W, 128), F32),
            pltpu.VMEM((2, 4 * W, C), F32),
            pltpu.VMEM((2, 4 * W, C), F32),
            pltpu.VMEM((2, 2, 4 * W, C), F32),
            pltpu.SemaphoreType.DMA((8,)),
        ],
        compiler_params=pltpu.CompilerParams(vmem_limit_bytes=32 * 2**20),
        name="decode",
    )(*operands)


def per_device(nt, nr, latent, entry_kernel, middle_kernel, upper_kernel):
    height = latent.shape[1]
    lat = jnp.transpose(latent, (0, 1, 3, 2))
    return decode(height * nr, height, *exchange(nt, nr, lat, entry_kernel, upper_kernel, middle_kernel))


def solution(mesh):
    nt = mesh.shape["tm"]
    nr = mesh.shape["rows"]
    return jax.shard_map(
        lambda *a: per_device(nt, nr, *a),
        mesh=mesh,
        in_specs=(P("tm", "rows", None, None), P(), P(), P()),
        out_specs=P("tm", "rows", None, None),
        check_vma=False,
    )
```
